32 devices in a mesh: row: 8 (over z, y), col: 4 (over x, core).
Axes of the slice: x: 2, y: 2, z: 4, core: 2. Of those that a mesh axis runs over, the one named last changes fastest.
Arguments:
- amplitudes: float32 [128, 512, 512], P(('row', 'col')), may hold values from -6 to 6
- integrals: float32 [512, 1024, 1024], P(('row', 'col')), may hold values from -0.01171875 to 0.01171875
- coupling: float32 [512, 32, 1024], P(('row', 'col')), may hold values from -0.046875 to 0.046875
- task_table: int32 [32, 16, 2], replicated, may hold values from -1 to 15, as said below
Outputs:
- residual: float32 [128, 1024], P(('row', 'col'))
The draws below stay inside these ranges and needn't reach their ends.
Inputs may be any that keep to these rules, and one draw needn't show every extreme that they name: `task_table`: every virtual tile pair (C, D), C and D in 0 to 15, appears in exactly one slot. In each device's row the valid slots come first and the rest hold -1 in both entries. Some device has all 16 slots valid and some device has none. `integrals`: slots that task_table marks -1 are not read.
All inputs are finite; a program needn't handle non-finite values.
Results may differ from the reference program's by a relative error of at most 0.0003.
Values sent between devices are 32-bit elements; how exact they have to be, the bound alone decides.
A program may use at most 192 MiB of HBM per device.

```python
import jax
import jax.numpy as jnp
from jax import lax

O = 32
V = 512
TB = 32
OW = 4
NVT = 16
TILES = 256
SLOTS = 16
SLOTS_ALL = 512
ROWS = 128
DEVICES = 32


def draw_task_table(key, part):
    first, second, third = jax.random.split(jax.random.fold_in(key, 11), 3)
    halves = DEVICES // 2
    split_sizes = jax.random.randint(first, (halves,), 0, SLOTS + 1).astype(jnp.int32)
    split_sizes = split_sizes.at[0].set(SLOTS)
    paired = jnp.stack([split_sizes, SLOTS - split_sizes], axis=1).reshape(DEVICES)
    device_order = jax.random.permutation(second, DEVICES)
    tallies = jnp.zeros((DEVICES,), jnp.int32).at[device_order].set(paired)
    offsets = jnp.cumsum(tallies) - tallies
    shuffled = jax.random.permutation(third, TILES).astype(jnp.int32)
    slot_range = jnp.arange(SLOTS, dtype=jnp.int32)
    positions = jnp.clip(offsets[:, None] + slot_range[None, :], 0, TILES - 1)
    valid = slot_range[None, :] < tallies[:, None]
    chosen = shuffled[positions]
    upper = jnp.where(valid, chosen // NVT, -1)
    lower = jnp.where(valid, chosen % NVT, -1)
    return jnp.stack([upper, lower], axis=-1).astype(jnp.int32)


def levels(rng, extent, cuts, smallest, largest):
    factor_of, own = 1.0, jax.random.fold_in(rng, 6)
    for position, shards_of in cuts:
        draws = jnp.exp(jax.random.uniform(jax.random.fold_in(own, position), (shards_of,), jnp.float32, smallest / len(cuts), largest / len(cuts)))
        factor_of = factor_of * jnp.repeat(draws, extent[position] // shards_of).reshape([-1 if axis == position else 1 for axis in range(len(extent))])
    return factor_of


def centred(own_key, shape, scale, reach, cuts=(), kind=jnp.bfloat16):
    factor_of = levels(own_key, shape, cuts, -0.22, 0.18) if cuts else 1.0
    values = jax.random.normal(own_key, shape, jnp.float32) * scale * factor_of
    return jnp.minimum(jnp.maximum(values, -reach), reach).astype(kind)


def setup_inputs(seed: int = 0) -> dict:
    arg_keys = jax.random.split(jax.random.key(seed), 5)
    amplitudes = centred(arg_keys[0], (ROWS, V, V), 1.0, 6.0, ((0, 32),), jnp.float32)
    integrals = centred(arg_keys[1], (SLOTS_ALL, TB * TB, TB * TB), (V * V) ** -0.5, 0.01171875, ((0, 32),), jnp.float32)
    coupling = centred(arg_keys[2], (V, O, O * TB), (V * O) ** -0.5, 0.046875, ((0, 32),), jnp.float32)
    task_table = draw_task_table(jax.random.fold_in(arg_keys[4], 71), 0)
    return dict(amplitudes=amplitudes, integrals=integrals, coupling=coupling, task_table=task_table)


def reference(amplitudes, integrals, coupling, task_table):
    flat = task_table.reshape(SLOTS_ALL, 2)
    valid = flat[:, 0] >= 0
    pair_ids = jnp.where(valid, flat[:, 0] * NVT + flat[:, 1], TILES).astype(jnp.int32)
    inverse = jnp.zeros((TILES + 1,), jnp.int32).at[pair_ids].set(jnp.arange(SLOTS_ALL, dtype=jnp.int32))[:TILES]

    def add_pair(partial_value, tile_index):
        upper = ((tile_index // NVT) * TB).astype(jnp.int32)
        lower = ((tile_index % NVT) * TB).astype(jnp.int32)
        columns = lax.dynamic_slice(amplitudes, (jnp.int32(0), upper, lower), (ROWS, TB, TB)).reshape(ROWS, TB * TB)
        integral_tile = integrals[inverse[tile_index]]
        product = lax.dot_general(columns, integral_tile, (((1,), (1,)), ((), ())), precision=lax.Precision.HIGHEST, preferred_element_type=jnp.float32)
        return partial_value + product, None

    ladder, _ = lax.scan(add_pair, jnp.zeros((ROWS, TB * TB), jnp.float32), jnp.arange(TILES, dtype=jnp.int32))
    regrouped = jnp.transpose(amplitudes[:, :TB, :].reshape(OW, O, TB, V), (0, 2, 3, 1)).reshape(OW * TB, V * O)
    hole_term = jnp.dot(regrouped, coupling.reshape(V * O, O * TB), precision=lax.Precision.HIGHEST, preferred_element_type=jnp.float32)
    hole_term = jnp.transpose(hole_term.reshape(OW, TB, O, TB), (0, 2, 1, 3)).reshape(ROWS, TB * TB)
    return ladder + hole_term
```

```python
import functools

import jax
import jax.numpy as jnp
from jax import lax
from jax.experimental import pallas as pl
from jax.experimental.pallas import tpu as pltpu
from jax.sharding import PartitionSpec as P

TB = 32
LANES = 128
GROUP = LANES // TB
SUB = TB * TB // LANES
MESH = pl.DeviceIdType.MESH


def chunk_transpose(x, chunk):
    a0 = jnp.where(chunk < 2, x[0], pltpu.roll(x[2], 2 * TB, 1))
    a2 = jnp.where(chunk < 2, pltpu.roll(x[0], 2 * TB, 1), x[2])
    a1 = jnp.where(chunk < 2, x[1], pltpu.roll(x[3], 2 * TB, 1))
    a3 = jnp.where(chunk < 2, pltpu.roll(x[1], 2 * TB, 1), x[3])
    even = chunk % 2 == 0
    y0 = jnp.where(even, a0, pltpu.roll(a1, TB, 1))
    y1 = jnp.where(even, pltpu.roll(a0, LANES - TB, 1), a1)
    y2 = jnp.where(even, a2, pltpu.roll(a3, TB, 1))
    y3 = jnp.where(even, pltpu.roll(a2, LANES - TB, 1), a3)
    return y0, y1, y2, y3


def exchange_kernel(
    cfg, list_ref, relay_ref, amp_ref, v_ref, out_ref,
    held, packed, send1, land, acc, stage, got, vbuf, flat, both, total,
    amp_sems, s1_send, s1_recv, s2_send, s2_recv, v_sems,
):
    planes, inner, ncol, local, slots, chunks, ct, cap_max, nvt = cfg
    members = inner * ncol
    wide = nvt * TB
    quads = wide // LANES
    depth = planes * local
    rows = members * depth
    per_chunk = slots // chunks
    row = lax.axis_index("row")
    col = lax.axis_index("col")
    z = row // inner
    me = (row % inner) * ncol + col

    copies = []
    for h in range(quads):
        for r in range(local):
            n = h * local + r
            copies.append(
                pltpu.make_async_copy(
                    amp_ref.at[r, :, pl.ds(h * LANES, LANES)],
                    held.at[pl.ds(n * wide, wide), :],
                    amp_sems.at[n],
                )
            )
    for copy in copies:
        copy.start()

    def fetch(t):
        return pltpu.make_async_copy(v_ref.at[slots - 1 - t], vbuf.at[t % 2], v_sems.at[t % 2])

    fetch(0).start()
    fetch(1).start()

    barrier = pltpu.get_barrier_semaphore()
    for d in range(1, planes):
        other = ((z + d) % planes) * inner + row % inner
        pl.semaphore_signal(barrier, inc=1, device_id=(other, col), device_id_type=MESH)
    for d in range(1, members):
        m = (me + d) % members
        pl.semaphore_signal(
            barrier, inc=1, device_id=(z * inner + m // ncol, m % ncol), device_id_type=MESH
        )

    total[...] = jnp.zeros_like(total)
    acc[0] = jnp.zeros(acc.shape[1:], jnp.float32)
    for copy in copies:
        copy.wait()

    lane_chunk = lax.broadcasted_iota(jnp.int32, (SUB, LANES), 1) // TB

    def pack_tile(upper, carry):
        for h in range(quads):
            for r in range(local):
                base = (h * local + r) * wide + upper * TB
                x = [held[pl.ds(base + j, SUB, stride=GROUP), :] for j in range(GROUP)]
                y = chunk_transpose(x, lane_chunk)
                for low in range(GROUP):
                    packed[upper * nvt + h * GROUP + low, r] = y[low]
        return carry

    lax.fori_loop(0, nvt, pack_tile, 0)

    def fill(k, carry):
        def one(t, c):
            for d in range(1, planes):
                tile = list_ref[((z + d) % planes) * cap_max + k * ct + t]
                send1[k, d - 1, t] = packed[tile]
            tile = list_ref[z * cap_max + k * ct + t]
            acc[1 + k * ct + t, pl.ds(z * local, local)] = packed[tile]
            return c

        return lax.fori_loop(0, ct, one, carry)

    def hop1(k, d):
        other = ((z + d) % planes) * inner + row % inner
        return pltpu.make_async_remote_copy(
            src_ref=send1.at[k, d - 1],
            dst_ref=land.at[k, d - 1],
            send_sem=s1_send.at[k, d - 1],
            recv_sem=s1_recv.at[k, d - 1],
            device_id=(other, col),
            device_id_type=MESH,
        )

    def hop2(r, d):
        m = (me + d) % members
        return pltpu.make_async_remote_copy(
            src_ref=stage.at[r, m],
            dst_ref=got.at[r, me],
            send_sem=s2_send.at[r, d - 1],
            recv_sem=s2_recv.at[r, d - 1],
            device_id=(z * inner + m // ncol, m % ncol),
            device_id_type=MESH,
        )

    def got_from(r, d):
        m = (me + members - d) % members
        return pltpu.make_async_remote_copy(
            src_ref=stage.at[r, m],
            dst_ref=got.at[r, m],
            send_sem=s2_send.at[r, d - 1],
            recv_sem=s2_recv.at[r, d - 1],
            device_id=(z * inner + m // ncol, m % ncol),
            device_id_type=MESH,
        )

    fill(0, 0)
    pl.semaphore_wait(barrier, planes + members - 2)

    def first(k, carry):
        fill(k, carry)
        for d in range(1, planes):
            hop1(k - 1, d).start()
        return carry

    lax.fori_loop(1, chunks, first, 0)
    for d in range(1, planes):
        hop1(chunks - 1, d).start()

    def ladder(r):
        for d in range(1, members):
            got_from(r, d).wait_recv()
        for m in range(members):
            for p in range(planes):
                flat[pl.ds((p * members + m) * local * SUB, local * SUB), :] = got[
                    r, m, pl.ds(p * local, local)
                ].reshape(local * SUB, LANES)
        for k in range(SUB):
            a = flat[pl.ds(k, rows, stride=SUB), :]
            high = a.astype(jnp.bfloat16)
            low = (a - high.astype(jnp.float32)).astype(jnp.bfloat16)
            both[pl.ds(0, rows), pl.ds(k * LANES, LANES)] = high
            both[pl.ds(rows, rows), pl.ds(k * LANES, LANES)] = low
        fetch(r).wait()
        dims = (((1,), (1,)), ((), ()))
        step = 256
        for i in range(TB * TB // step):
            part = pl.ds(i * step, step)
            v = vbuf[r % 2, part, :]
            vh = v.astype(jnp.bfloat16)
            vl = (v - vh.astype(jnp.float32)).astype(jnp.bfloat16)
            b = both[...]
            total[part, :] += lax.dot_general(
                vh, b, dims, preferred_element_type=jnp.float32
            ) + lax.dot_general(vl, b, dims, preferred_element_type=jnp.float32)

        @pl.when(r + 2 < slots)
        def _():
            fetch(r + 2).start()

    def ladders(k):
        def one(i, c):
            ladder(k * per_chunk + i)
            return c

        lax.fori_loop(0, per_chunk, one, 0)

    def step(k, carry):
        @pl.when(k < chunks)
        def _():
            for d in range(1, planes):
                source = (z + planes - d) % planes
                hop1(k, d).wait_recv()
                acc[pl.ds(1 + k * ct, ct), pl.ds(source * local, local)] = land[k, d - 1]
            for i in range(per_chunk):
                r = k * per_chunk + i

                def one(m, c):
                    stage[r, m] = acc[relay_ref[r * members + m]]
                    return c

                lax.fori_loop(0, members, one, 0)
            for i in range(per_chunk):
                r = k * per_chunk + i
                got[r, me] = acc[relay_ref[r * members + me]]
            for i in range(per_chunk):
                for d in range(1, members):
                    hop2(k * per_chunk + i, d).start()

        @pl.when(k > 0)
        def _():
            ladders(k - 1)

        return carry

    lax.fori_loop(0, chunks + 1, step, 0)

    def drain1(k, carry):
        for d in range(1, planes):
            hop1(k, d).wait_send()
        return carry

    def drain2(r, carry):
        for d in range(1, members):
            hop2(r, d).wait_send()
        return carry

    lax.fori_loop(0, chunks, drain1, 0)
    lax.fori_loop(0, slots, drain2, 0)
    out_ref[...] = (total[:, :rows] + total[:, rows:]).T


def exchange(planes, inner, ncol, chunks, ct, cap_max, tag, lists, relay, amplitudes, integrals):
    local, wide, _ = amplitudes.shape
    slots, size, _ = integrals.shape
    members = inner * ncol
    nvt = wide // TB
    quads = wide // LANES
    depth = planes * local
    rows = members * depth
    cfg = (planes, inner, ncol, local, slots, chunks, ct, cap_max, nvt)
    f32 = jnp.float32
    return pl.pallas_call(
        functools.partial(exchange_kernel, cfg),
        out_shape=jax.ShapeDtypeStruct((rows, size), f32),
        in_specs=[
            pl.BlockSpec(memory_space=pltpu.SMEM),
            pl.BlockSpec(memory_space=pltpu.SMEM),
            pl.BlockSpec(memory_space=pl.ANY),
            pl.BlockSpec(memory_space=pl.ANY),
        ],
        out_specs=pl.BlockSpec(memory_space=pltpu.VMEM),
        scratch_shapes=[
            pltpu.VMEM((quads * local * wide, LANES), f32),
            pltpu.VMEM((nvt * nvt, local, SUB, LANES), f32),
            pltpu.VMEM((chunks, planes - 1, ct, local, SUB, LANES), f32),
            pltpu.VMEM((chunks, planes - 1, ct, local, SUB, LANES), f32),
            pltpu.VMEM((chunks * ct + 1, depth, SUB, LANES), f32),
            pltpu.VMEM((slots, members, depth, SUB, LANES), f32),
            pltpu.VMEM((slots, members, depth, SUB, LANES), f32),
            pltpu.VMEM((2, size, size), f32),
            pltpu.VMEM((rows * SUB, LANES), f32),
            pltpu.VMEM((2 * rows, size), jnp.bfloat16),
            pltpu.VMEM((size, 2 * rows), f32),
            pltpu.SemaphoreType.DMA((quads * local,)),
            pltpu.SemaphoreType.DMA((chunks, planes - 1)),
            pltpu.SemaphoreType.DMA((chunks, planes - 1)),
            pltpu.SemaphoreType.DMA((slots, members - 1)),
            pltpu.SemaphoreType.DMA((slots, members - 1)),
            pltpu.SemaphoreType.DMA((2,)),
        ],
        compiler_params=pltpu.CompilerParams(
            collective_id=tag, has_side_effects=True, vmem_limit_bytes=63 * 1024 * 1024
        ),
        name="exchange",
    )(lists, relay, amplitudes, integrals)


def tables(task_table, planes, members, z, nvt):
    slots = task_table.shape[1]
    upper, lower = task_table[:, :, 0], task_table[:, :, 1]
    ids = jnp.where(upper >= 0, upper * nvt + lower, -1).reshape(planes, members, slots)
    order = jnp.transpose(ids[:, :, ::-1], (0, 2, 1)).reshape(planes, slots * members)
    valid = (order >= 0).astype(jnp.int32)
    place = jnp.cumsum(valid, axis=1)
    fullest = jnp.max(place[:, -1])
    cap_max = slots * members
    at = jnp.arange(1, cap_max + 1, dtype=jnp.int32)
    hit = (place[:, None, :] == at[None, :, None]) & (valid[:, None, :] > 0)
    lists = jnp.sum(jnp.where(hit, order[:, None, :], 0), axis=2)
    relay = lax.dynamic_index_in_dim(place * valid, z, 0, keepdims=False)
    return lists.reshape(-1), relay, fullest


def body(amplitudes, integrals, coupling, task_table):
    nrow, ncol = lax.axis_size("row"), lax.axis_size("col")
    devices_all = nrow * ncol
    local_rows, wide, _ = amplitudes.shape
    slots = integrals.shape[0]
    total_rows = devices_all * local_rows
    nvt = wide // TB
    inner = 2
    planes = nrow // inner
    members = inner * ncol
    z = lax.axis_index("row") // inner

    first_tile = amplitudes[:, :TB, :]
    pieces = lax.all_to_all(first_tile, ("row", "col"), split_axis=2, concat_axis=0, tiled=True)

    lists, relay, fullest = tables(task_table, planes, members, z, nvt)
    cap_max = slots * members
    mean = nvt * nvt // planes
    chunks = max(slots // 2, 1)
    unit = mean // chunks
    sizes = sorted({unit + -(-unit * n // 8) for n in (1, 2, 3, 4, 6, 8)})
    branches = [
        functools.partial(exchange, planes, inner, ncol, chunks, ct, cap_max, tag)
        for tag, ct in enumerate(sizes)
    ]
    limits = jnp.array([ct * chunks for ct in sizes[:-1]], jnp.int32)
    pick = jnp.sum((fullest > limits).astype(jnp.int32))
    ladder = lax.switch(pick, branches, lists, relay, amplitudes, integrals)

    width_part = pieces.shape[2]
    occupied = coupling.shape[1]
    window = total_rows // occupied
    regrouped = jnp.transpose(
        pieces.reshape(window, occupied, TB, width_part), (0, 2, 3, 1)
    ).reshape(window * TB, width_part * occupied)
    coupling_rows = coupling.reshape(width_part * occupied, occupied * TB)
    hole_term = jnp.dot(
        regrouped,
        coupling_rows,
        precision=lax.Precision.HIGHEST,
        preferred_element_type=jnp.float32,
    )
    hole_term = jnp.transpose(hole_term.reshape(window, TB, occupied, TB), (0, 2, 1, 3)).reshape(
        total_rows, TB * TB
    )
    partial = (ladder + hole_term).reshape(devices_all, local_rows * SUB, LANES)
    shares = lax.all_to_all(partial, ("row", "col"), split_axis=0, concat_axis=0, tiled=True)
    return jnp.sum(shares, axis=0).reshape(local_rows, TB * TB)


def solution(mesh):
    in_specs = (
        P(("row", "col"), None, None),
        P(("row", "col"), None, None),
        P(("row", "col"), None, None),
        P(),
    )
    out_specs = P(("row", "col"), None)
    return jax.shard_map(body, mesh=mesh, in_specs=in_specs, out_specs=out_specs, check_vma=False)
```

```python
import functools

import jax
import jax.numpy as jnp
from jax import lax
from jax.experimental import pallas as pl
from jax.experimental.pallas import tpu as pltpu
from jax.sharding import PartitionSpec as P

TB = 32
LANES = 128
GROUP = LANES // TB
SUB = TB * TB // LANES
MESH = pl.DeviceIdType.MESH


def chunk_transpose(x, chunk):
    a0 = jnp.where(chunk < 2, x[0], pltpu.roll(x[2], 2 * TB, 1))
    a2 = jnp.where(chunk < 2, pltpu.roll(x[0], 2 * TB, 1), x[2])
    a1 = jnp.where(chunk < 2, x[1], pltpu.roll(x[3], 2 * TB, 1))
    a3 = jnp.where(chunk < 2, pltpu.roll(x[1], 2 * TB, 1), x[3])
    even = chunk % 2 == 0
    y0 = jnp.where(even, a0, pltpu.roll(a1, TB, 1))
    y1 = jnp.where(even, pltpu.roll(a0, LANES - TB, 1), a1)
    y2 = jnp.where(even, a2, pltpu.roll(a3, TB, 1))
    y3 = jnp.where(even, pltpu.roll(a2, LANES - TB, 1), a3)
    return y0, y1, y2, y3


def exchange_kernel(
    cfg, list_ref, relay_ref, amp_ref, v_ref, w_ref, out_ref,
    held, packed, send1, land, acc, stage, got, vbuf, flat, both, total,
    hole_in, turned, weights, product, hole_sum, shares, plane_in, plane_sum, line_in, final,
    amp_sems, s1_send, s1_recv, s2_send, s2_recv, v_sems,
    h_send, h_recv, w_send, w_recv, w_own, a_send, a_recv, b_send, b_recv,
):
    planes, inner, ncol, local, slots, chunks, ct, cap_max, nvt, sharers = cfg
    members = inner * ncol
    wide = nvt * TB
    quads = wide // LANES
    unit = local * SUB
    depth = planes * unit
    rows = members * planes * local
    halves = ((0, ct - ct // 2), (ct - ct // 2, ct // 2))
    row = lax.axis_index("row")
    col = lax.axis_index("col")
    z = row // inner
    me = (row % inner) * ncol + col
    index = row * ncol + col
    tile_me = index // sharers
    share = index % sharers

    def place(n):
        return (n // ncol, n % ncol)

    def in_plane(m):
        return (z * inner + m // ncol, m % ncol)

    def in_line(p):
        return (p * inner + row % inner, col)

    def to_class(e):
        return place(((tile_me + e) % nvt) * sharers + share)

    copies = []
    for h in range(quads):
        for r in range(local):
            n = h * local + r
            copies.append(
                pltpu.make_async_copy(
                    amp_ref.at[r, :, pl.ds(h * LANES, LANES)],
                    held.at[pl.ds(n * wide, wide), :],
                    amp_sems.at[n],
                )
            )
    for copy in copies:
        copy.start()

    def fetch(t):
        return pltpu.make_async_copy(v_ref.at[slots - 1 - t], vbuf.at[t % 2], v_sems.at[t % 2])

    hole_in[...] = jnp.zeros_like(hole_in)
    barrier = pltpu.get_barrier_semaphore()
    for e in range(1, nvt):
        pl.semaphore_signal(barrier, inc=1, device_id=to_class(e), device_id_type=MESH)
    for d in range(1, members):
        pl.semaphore_signal(
            barrier, inc=1, device_id=in_plane((me + d) % members), device_id_type=MESH
        )

    total[...] = jnp.zeros_like(total)
    acc[0] = jnp.zeros(acc.shape[1:], jnp.float32)
    own_weights = pltpu.make_async_copy(w_ref, weights.at[share], w_own)
    for copy in copies:
        copy.wait()
    own_weights.start()
    fetch(0).start()
    fetch(1).start()

    lane_chunk = lax.broadcasted_iota(jnp.int32, (SUB, LANES), 1) // TB

    def pack_tile(upper, carry):
        for h in range(quads):
            for r in range(local):
                base = (h * local + r) * wide + upper * TB
                x = [held[pl.ds(base + j, SUB, stride=GROUP), :] for j in range(GROUP)]
                y = chunk_transpose(x, lane_chunk)
                for low in range(GROUP):
                    packed[upper * nvt + h * GROUP + low, pl.ds(r * SUB, SUB), :] = y[low]
        return carry

    lax.fori_loop(0, nvt, pack_tile, 0)

    def fill(k, carry):
        def one(t, c):
            for d in range(1, planes):
                tile = list_ref[((z + d) % planes) * cap_max + k * ct + t]
                send1[k, d - 1, t] = packed[tile]
            tile = list_ref[z * cap_max + k * ct + t]
            acc[1 + k * ct + t, pl.ds(z * unit, unit), :] = packed[tile]
            return c

        return lax.fori_loop(0, ct, one, carry)

    def hop1(k, i, d):
        part = pl.ds(halves[i][0], halves[i][1])
        return pltpu.make_async_remote_copy(
            src_ref=send1.at[k, d - 1, part],
            dst_ref=land.at[k, d - 1, part],
            send_sem=s1_send.at[k, i, d - 1],
            recv_sem=s1_recv.at[k, i, d - 1],
            device_id=in_line((z + d) % planes),
            device_id_type=MESH,
        )

    def hop2(r, d):
        m = (me + d) % members
        return pltpu.make_async_remote_copy(
            src_ref=stage.at[r, m],
            dst_ref=got.at[r, me],
            send_sem=s2_send.at[r, d - 1],
            recv_sem=s2_recv.at[r, d - 1],
            device_id=in_plane(m),
            device_id_type=MESH,
        )

    def got_from(r, d):
        m = (me + members - d) % members
        return pltpu.make_async_remote_copy(
            src_ref=stage.at[r, m],
            dst_ref=got.at[r, m],
            send_sem=s2_send.at[r, d - 1],
            recv_sem=s2_recv.at[r, d - 1],
            device_id=in_plane(m),
            device_id_type=MESH,
        )

    def hole_out(e):
        return pltpu.make_async_remote_copy(
            src_ref=packed.at[(tile_me + e) % nvt],
            dst_ref=hole_in.at[pl.ds(pl.multiple_of(index * unit, unit), unit), :],
            send_sem=h_send.at[e - 1],
            recv_sem=h_recv.at[e - 1],
            device_id=to_class(e),
            device_id_type=MESH,
        )

    def hole_from(e):
        source = ((tile_me + nvt - e) % nvt) * sharers + share
        return pltpu.make_async_remote_copy(
            src_ref=packed.at[0],
            dst_ref=hole_in.at[pl.ds(pl.multiple_of(source * unit, unit), unit), :],
            send_sem=h_send.at[e - 1],
            recv_sem=h_recv.at[e - 1],
            device_id=place(source),
            device_id_type=MESH,
        )

    def weights_out(e):
        return pltpu.make_async_remote_copy(
            src_ref=weights.at[share],
            dst_ref=weights.at[share],
            send_sem=w_send.at[e - 1],
            recv_sem=w_recv.at[e - 1],
            device_id=place(tile_me * sharers + (share + e) % sharers),
            device_id_type=MESH,
        )

    def weights_from(e):
        other = (share + sharers - e) % sharers
        return pltpu.make_async_remote_copy(
            src_ref=weights.at[other],
            dst_ref=weights.at[other],
            send_sem=w_send.at[e - 1],
            recv_sem=w_recv.at[e - 1],
            device_id=place(tile_me * sharers + other),
            device_id_type=MESH,
        )

    fill(0, 0)
    pl.semaphore_wait(barrier, nvt + members - 2)

    def launch(k):
        for i in range(2):
            for d in range(1, planes):
                hop1(k, i, d).start()

    def first(k, carry):
        fill(k, carry)
        launch(k - 1)
        return carry

    first(1, 0)
    for e in range(1, nvt):
        hole_out(e).start()
    lax.fori_loop(2, chunks, first, 0)
    launch(chunks - 1)
    hole_in[pl.ds(pl.multiple_of(index * unit, unit), unit), :] = packed[tile_me]
    own_weights.wait()
    for e in range(1, sharers):
        weights_out(e).start()

    def split():
        for k in range(SUB):
            a = flat[pl.ds(k, rows, stride=SUB), :]
            high = a.astype(jnp.bfloat16)
            low = (a - high.astype(jnp.float32)).astype(jnp.bfloat16)
            both[pl.ds(0, rows), pl.ds(k * LANES, LANES)] = high
            both[pl.ds(rows, rows), pl.ds(k * LANES, LANES)] = low

    def hole():
        for e in range(1, nvt):
            hole_from(e).wait_recv()
        for e in range(1, sharers):
            weights_from(e).wait_recv()
        for s in range(SUB):
            turned[...] = hole_in[pl.ds(s, rows, stride=SUB), :].T
            for j in range(GROUP):
                x = [turned[pl.ds(j * TB + n, SUB, stride=GROUP), :] for n in range(GROUP)]
                y = chunk_transpose(x, lane_chunk)
                for i in range(rows // TB):
                    flat[pl.ds((i * TB + GROUP * s + j) * SUB, SUB), :] = y[i]
        split()
        span = 2 * LANES
        for n in range(TB * TB // span):
            out = jnp.zeros((2 * rows, span), jnp.float32)
            for g in range(sharers):
                width = weights.shape[1]
                w = weights[g, :, pl.ds(n * span, span)]
                wh = w.astype(jnp.bfloat16)
                wl = (w - wh.astype(jnp.float32)).astype(jnp.bfloat16)
                b = both[:, pl.ds(g * width, width)]
                out += jnp.dot(b, wh, preferred_element_type=jnp.float32) + jnp.dot(
                    b, wl, preferred_element_type=jnp.float32
                )
            out = out[:rows] + out[rows:]
            product[pl.ds(2 * n * rows, rows), :] = out[:, :LANES]
            product[pl.ds((2 * n + 1) * rows, rows), :] = out[:, LANES:]
        for i in range(rows // TB):
            for q in range(TB // GROUP):
                x = [
                    product[pl.ds(q * rows + i * TB + n, SUB, stride=GROUP), :]
                    for n in range(GROUP)
                ]
                y = chunk_transpose(x, lane_chunk)
                for low in range(GROUP):
                    owner, r = divmod(i * TB + q * GROUP + low, local)
                    at = ((owner % members) * planes + owner // members) * local + r
                    hole_sum[pl.ds(at * SUB, SUB), :] = y[low]

    def ladder(r):
        for d in range(1, members):
            got_from(r, d).wait_recv()
        for m in range(members):
            flat[pl.ds(m * depth, depth), :] = got[r, m]
        split()
        fetch(r).wait()
        dims = (((1,), (1,)), ((), ()))
        step = 256
        for i in range(TB * TB // step):
            part = pl.ds(i * step, step)
            v = vbuf[r % 2, part, :]
            vh = v.astype(jnp.bfloat16)
            vl = (v - vh.astype(jnp.float32)).astype(jnp.bfloat16)
            b = both[...]
            total[part, :] += lax.dot_general(
                vh, b, dims, preferred_element_type=jnp.float32
            ) + lax.dot_general(vl, b, dims, preferred_element_type=jnp.float32)

        @pl.when(r + 2 < slots)
        def _():
            fetch(r + 2).start()

    def step(k, carry):
        @pl.when(k < chunks)
        def _():
            for i in range(2):
                start, count = halves[i]
                for d in range(1, planes):
                    source = (z + planes - d) % planes
                    hop1(k, i, d).wait_recv()
                    acc[
                        pl.ds(1 + k * ct + start, count),
                        pl.ds(pl.multiple_of(source * unit, unit), unit),
                        :,
                    ] = land[k, d - 1, pl.ds(start, count)]
                r = 2 * k + i

                def one(m, c):
                    stage[r, m] = acc[relay_ref[r * members + m]]
                    return c

                lax.fori_loop(0, members, one, 0)
                got[r, me] = acc[relay_ref[r * members + me]]
                for d in range(1, members):
                    hop2(r, d).start()

        @pl.when(k == chunks // 2)
        def _():
            hole()

        @pl.when(k > 0)
        def _():
            def one(i, c):
                ladder(2 * k - 2 + i)
                return c

            lax.fori_loop(0, 2, one, 0)

        return carry

    lax.fori_loop(0, chunks + 1, step, 0)

    for s in range(SUB):
        part = pl.ds(s * LANES, LANES)
        t = (total[part, :rows] + total[part, rows:]).T
        shares[pl.ds(s, rows, stride=SUB), :] = t + hole_sum[pl.ds(s, rows, stride=SUB), :]

    def plane_out(d):
        m = (me + d) % members
        return pltpu.make_async_remote_copy(
            src_ref=shares.at[pl.ds(pl.multiple_of(m * depth, depth), depth), :],
            dst_ref=plane_in.at[d - 1],
            send_sem=a_send.at[d - 1],
            recv_sem=a_recv.at[d - 1],
            device_id=in_plane(m),
            device_id_type=MESH,
        )

    def line_out(d):
        p = (z + d) % planes
        return pltpu.make_async_remote_copy(
            src_ref=plane_sum.at[pl.ds(pl.multiple_of(p * unit, unit), unit), :],
            dst_ref=line_in.at[d - 1],
            send_sem=b_send.at[d - 1],
            recv_sem=b_recv.at[d - 1],
            device_id=in_line(p),
            device_id_type=MESH,
        )

    for d in range(1, members):
        plane_out(d).start()
    value = shares[pl.ds(pl.multiple_of(me * depth, depth), depth), :]
    for d in range(1, members):
        plane_out(d).wait_recv()
        value += plane_in[d - 1]
    plane_sum[...] = value
    for d in range(1, planes):
        line_out(d).start()

    def drain1(k, carry):
        for i in range(2):
            for d in range(1, planes):
                hop1(k, i, d).wait_send()
        return carry

    def drain2(r, carry):
        for d in range(1, members):
            hop2(r, d).wait_send()
        return carry

    lax.fori_loop(0, chunks, drain1, 0)
    lax.fori_loop(0, slots, drain2, 0)
    for e in range(1, nvt):
        hole_out(e).wait_send()
    for e in range(1, sharers):
        weights_out(e).wait_send()
    for d in range(1, members):
        plane_out(d).wait_send()
    value = plane_sum[pl.ds(pl.multiple_of(z * unit, unit), unit), :]
    for d in range(1, planes):
        line_out(d).wait_recv()
        value += line_in[d - 1]
    final[...] = value
    for s in range(SUB):
        out_ref[:, pl.ds(s * LANES, LANES)] = final[pl.ds(s, local, stride=SUB), :]
    for d in range(1, planes):
        line_out(d).wait_send()


def exchange(
    planes, inner, ncol, chunks, ct, cap_max, tag, lists, relay, amplitudes, integrals, coupling
):
    local, wide, _ = amplitudes.shape
    slots, size, _ = integrals.shape
    members = inner * ncol
    nvt = wide // TB
    quads = wide // LANES
    unit = local * SUB
    depth = planes * unit
    rows = members * planes * local
    held_weights = coupling.shape[0]
    sharers = size // held_weights
    cfg = (planes, inner, ncol, local, slots, chunks, ct, cap_max, nvt, sharers)
    f32 = jnp.float32
    dma = pltpu.SemaphoreType.DMA
    return pl.pallas_call(
        functools.partial(exchange_kernel, cfg),
        out_shape=jax.ShapeDtypeStruct((local, size), f32),
        in_specs=[
            pl.BlockSpec(memory_space=pltpu.SMEM),
            pl.BlockSpec(memory_space=pltpu.SMEM),
            pl.BlockSpec(memory_space=pl.ANY),
            pl.BlockSpec(memory_space=pl.ANY),
            pl.BlockSpec(memory_space=pl.ANY),
        ],
        out_specs=pl.BlockSpec(memory_space=pltpu.VMEM),
        scratch_shapes=[
            pltpu.VMEM((quads * local * wide, LANES), f32),
            pltpu.VMEM((nvt * nvt, unit, LANES), f32),
            pltpu.VMEM((chunks, planes - 1, ct, unit, LANES), f32),
            pltpu.VMEM((chunks, planes - 1, ct, unit, LANES), f32),
            pltpu.VMEM((chunks * ct + 1, depth, LANES), f32),
            pltpu.VMEM((slots, members, depth, LANES), f32),
            pltpu.VMEM((slots, members, depth, LANES), f32),
            pltpu.VMEM((2, size, size), f32),
            pltpu.VMEM((rows * SUB, LANES), f32),
            pltpu.VMEM((2 * rows, size), jnp.bfloat16),
            pltpu.VMEM((size, 2 * rows), f32),
            pltpu.VMEM((rows * SUB, LANES), f32),
            pltpu.VMEM((LANES, rows), f32),
            pltpu.VMEM((sharers, held_weights, size), f32),
            pltpu.VMEM((rows * SUB, LANES), f32),
            pltpu.VMEM((rows * SUB, LANES), f32),
            pltpu.VMEM((rows * SUB, LANES), f32),
            pltpu.VMEM((members - 1, depth, LANES), f32),
            pltpu.VMEM((depth, LANES), f32),
            pltpu.VMEM((planes - 1, unit, LANES), f32),
            pltpu.VMEM((unit, LANES), f32),
            dma((quads * local,)),
            dma((chunks, 2, planes - 1)),
            dma((chunks, 2, planes - 1)),
            dma((slots, members - 1)),
            dma((slots, members - 1)),
            dma((2,)),
            dma((nvt - 1,)),
            dma((nvt - 1,)),
            dma((max(sharers - 1, 1),)),
            dma((max(sharers - 1, 1),)),
            dma(()),
            dma((members - 1,)),
            dma((members - 1,)),
            dma((planes - 1,)),
            dma((planes - 1,)),
        ],
        compiler_params=pltpu.CompilerParams(
            collective_id=tag, has_side_effects=True, vmem_limit_bytes=67043328
        ),
        name="exchange",
    )(lists, relay, amplitudes, integrals, coupling)


def tables(task_table, planes, members, z, nvt):
    slots = task_table.shape[1]
    upper, lower = task_table[:, :, 0], task_table[:, :, 1]
    ids = jnp.where(upper >= 0, upper * nvt + lower, -1).reshape(planes, members, slots)
    order = jnp.transpose(ids[:, :, ::-1], (0, 2, 1)).reshape(planes, slots * members)
    valid = (order >= 0).astype(jnp.int32)
    place = jnp.cumsum(valid, axis=1)
    fullest = jnp.max(place[:, -1])
    cap_max = slots * members
    at = jnp.arange(1, cap_max + 1, dtype=jnp.int32)
    hit = (place[:, None, :] == at[None, :, None]) & (valid[:, None, :] > 0)
    lists = jnp.sum(jnp.where(hit, order[:, None, :], 0), axis=2)
    relay = lax.dynamic_index_in_dim(place * valid, z, 0, keepdims=False)
    return lists.reshape(-1), relay, fullest


def body(amplitudes, integrals, coupling, task_table):
    nrow, ncol = lax.axis_size("row"), lax.axis_size("col")
    wide = amplitudes.shape[1]
    slots, size, _ = integrals.shape
    nvt = wide // TB
    inner = 2
    planes = nrow // inner
    members = inner * ncol
    z = lax.axis_index("row") // inner

    lists, relay, fullest = tables(task_table, planes, members, z, nvt)
    cap_max = slots * members
    mean = nvt * nvt // planes
    chunks = slots // 2
    unit = mean // chunks
    sizes = sorted({unit + -(-unit * n // 8) for n in (1, 2, 3, 4, 6, 8)})
    branches = [
        functools.partial(exchange, planes, inner, ncol, chunks, ct, cap_max, tag)
        for tag, ct in enumerate(sizes)
    ]
    limits = jnp.array([ct * chunks for ct in sizes[:-1]], jnp.int32)
    pick = jnp.sum((fullest > limits).astype(jnp.int32))
    return lax.switch(
        pick, branches, lists, relay, amplitudes, integrals, coupling.reshape(-1, size)
    )


def solution(mesh):
    in_specs = (
        P(("row", "col"), None, None),
        P(("row", "col"), None, None),
        P(("row", "col"), None, None),
        P(),
    )
    out_specs = P(("row", "col"), None)
    return jax.shard_map(body, mesh=mesh, in_specs=in_specs, out_specs=out_specs, check_vma=False)
```

```python
import functools

import jax
import jax.numpy as jnp
from jax import lax
from jax.experimental import pallas as pl
from jax.experimental.pallas import tpu as pltpu
from jax.sharding import PartitionSpec as P

TB = 32
LANES = 128
GROUP = LANES // TB
SUB = TB * TB // LANES
MESH = pl.DeviceIdType.MESH


def chunk_transpose(x, chunk):
    a0 = jnp.where(chunk < 2, x[0], pltpu.roll(x[2], 2 * TB, 1))
    a2 = jnp.where(chunk < 2, pltpu.roll(x[0], 2 * TB, 1), x[2])
    a1 = jnp.where(chunk < 2, x[1], pltpu.roll(x[3], 2 * TB, 1))
    a3 = jnp.where(chunk < 2, pltpu.roll(x[1], 2 * TB, 1), x[3])
    even = chunk % 2 == 0
    y0 = jnp.where(even, a0, pltpu.roll(a1, TB, 1))
    y1 = jnp.where(even, pltpu.roll(a0, LANES - TB, 1), a1)
    y2 = jnp.where(even, a2, pltpu.roll(a3, TB, 1))
    y3 = jnp.where(even, pltpu.roll(a2, LANES - TB, 1), a3)
    return y0, y1, y2, y3


def exchange_kernel(
    cfg, list_ref, relay_ref, amp_ref, v_ref, w_ref, out_ref,
    held, packed, send1, land, acc, stage, got, vbuf, flat, both, total,
    hole_in, turned, weights, product, hole_sum, shares, plane_in, plane_sum, line_in, final,
    amp_sems, s1_send, s1_recv, s2_send, s2_recv, v_sems,
    h_send, h_recv, w_send, w_recv, w_own, a_send, a_recv, b_send, b_recv,
):
    planes, inner, ncol, local, slots, chunks, ct, cap_max, nvt, sharers = cfg
    members = inner * ncol
    wide = nvt * TB
    quads = wide // LANES
    unit = local * SUB
    depth = planes * unit
    rows = members * planes * local
    halves = ((0, ct - ct // 2), (ct - ct // 2, ct // 2))
    row = lax.axis_index("row")
    col = lax.axis_index("col")
    z = row // inner
    me = (row % inner) * ncol + col
    index = row * ncol + col
    tile_me = index // sharers
    share = index % sharers

    def place(n):
        return (n // ncol, n % ncol)

    def in_plane(m):
        return (z * inner + m // ncol, m % ncol)

    def in_line(p):
        return (p * inner + row % inner, col)

    def to_class(e):
        return place(((tile_me + e) % nvt) * sharers + share)

    copies = []
    for h in range(quads):
        for r in range(local):
            n = h * local + r
            copies.append(
                pltpu.make_async_copy(
                    amp_ref.at[r, :, pl.ds(h * LANES, LANES)],
                    held.at[pl.ds(n * wide, wide), :],
                    amp_sems.at[n],
                )
            )
    for copy in copies:
        copy.start()

    def fetch(t):
        return pltpu.make_async_copy(v_ref.at[slots - 1 - t], vbuf.at[t % 2], v_sems.at[t % 2])

    hole_in[...] = jnp.zeros_like(hole_in)
    barrier = pltpu.get_barrier_semaphore()
    for e in range(1, nvt):
        pl.semaphore_signal(barrier, inc=1, device_id=to_class(e), device_id_type=MESH)
    for d in range(1, members):
        pl.semaphore_signal(
            barrier, inc=1, device_id=in_plane((me + d) % members), device_id_type=MESH
        )

    total[...] = jnp.zeros_like(total)
    acc[0] = jnp.zeros(acc.shape[1:], jnp.float32)
    own_weights = pltpu.make_async_copy(w_ref, weights.at[share], w_own)
    for copy in copies:
        copy.wait()
    own_weights.start()
    fetch(0).start()
    fetch(1).start()

    lane_chunk = lax.broadcasted_iota(jnp.int32, (SUB, LANES), 1) // TB

    def pack_tile(upper, carry):
        for h in range(quads):
            for r in range(local):
                base = (h * local + r) * wide + upper * TB
                x = [held[pl.ds(base + j, SUB, stride=GROUP), :] for j in range(GROUP)]
                y = chunk_transpose(x, lane_chunk)
                for low in range(GROUP):
                    packed[upper * nvt + h * GROUP + low, pl.ds(r * SUB, SUB), :] = y[low]
        return carry

    lax.fori_loop(0, nvt, pack_tile, 0)

    def fill(k, carry):
        def one(t, c):
            for d in range(1, planes):
                tile = list_ref[((z + d) % planes) * cap_max + k * ct + t]
                send1[k, d - 1, t] = packed[tile]
            tile = list_ref[z * cap_max + k * ct + t]
            acc[1 + k * ct + t, pl.ds(z * unit, unit), :] = packed[tile]
            return c

        return lax.fori_loop(0, ct, one, carry)

    def hop1(k, i, d):
        part = pl.ds(halves[i][0], halves[i][1])
        return pltpu.make_async_remote_copy(
            src_ref=send1.at[k, d - 1, part],
            dst_ref=land.at[k, d - 1, part],
            send_sem=s1_send.at[k, i, d - 1],
            recv_sem=s1_recv.at[k, i, d - 1],
            device_id=in_line((z + d) % planes),
            device_id_type=MESH,
        )

    def hop2(r, d):
        m = (me + d) % members
        return pltpu.make_async_remote_copy(
            src_ref=stage.at[r, m],
            dst_ref=got.at[r, me],
            send_sem=s2_send.at[r, d - 1],
            recv_sem=s2_recv.at[r, d - 1],
            device_id=in_plane(m),
            device_id_type=MESH,
        )

    def got_from(r, d):
        m = (me + members - d) % members
        return pltpu.make_async_remote_copy(
            src_ref=stage.at[r, m],
            dst_ref=got.at[r, m],
            send_sem=s2_send.at[r, d - 1],
            recv_sem=s2_recv.at[r, d - 1],
            device_id=in_plane(m),
            device_id_type=MESH,
        )

    def hole_out(e):
        return pltpu.make_async_remote_copy(
            src_ref=packed.at[(tile_me + e) % nvt],
            dst_ref=hole_in.at[pl.ds(pl.multiple_of(index * unit, unit), unit), :],
            send_sem=h_send.at[e - 1],
            recv_sem=h_recv.at[e - 1],
            device_id=to_class(e),
            device_id_type=MESH,
        )

    def hole_from(e):
        source = ((tile_me + nvt - e) % nvt) * sharers + share
        return pltpu.make_async_remote_copy(
            src_ref=packed.at[0],
            dst_ref=hole_in.at[pl.ds(pl.multiple_of(source * unit, unit), unit), :],
            send_sem=h_send.at[e - 1],
            recv_sem=h_recv.at[e - 1],
            device_id=place(source),
            device_id_type=MESH,
        )

    def weights_out(e):
        return pltpu.make_async_remote_copy(
            src_ref=weights.at[share],
            dst_ref=weights.at[share],
            send_sem=w_send.at[e - 1],
            recv_sem=w_recv.at[e - 1],
            device_id=place(tile_me * sharers + (share + e) % sharers),
            device_id_type=MESH,
        )

    def weights_from(e):
        other = (share + sharers - e) % sharers
        return pltpu.make_async_remote_copy(
            src_ref=weights.at[other],
            dst_ref=weights.at[other],
            send_sem=w_send.at[e - 1],
            recv_sem=w_recv.at[e - 1],
            device_id=place(tile_me * sharers + other),
            device_id_type=MESH,
        )

    fill(0, 0)
    pl.semaphore_wait(barrier, nvt + members - 2)

    fill(1, 0)
    for i in range(2):
        for d in range(1, planes):
            hop1(0, i, d).start()
    for e in range(1, nvt):
        hole_out(e).start()
    lax.fori_loop(2, chunks, fill, 0)
    hole_in[pl.ds(pl.multiple_of(index * unit, unit), unit), :] = packed[tile_me]
    own_weights.wait()
    for e in range(1, sharers):
        weights_out(e).start()

    def split():
        for k in range(SUB):
            a = flat[pl.ds(k, rows, stride=SUB), :]
            high = a.astype(jnp.bfloat16)
            low = (a - high.astype(jnp.float32)).astype(jnp.bfloat16)
            both[pl.ds(0, rows), pl.ds(k * LANES, LANES)] = high
            both[pl.ds(rows, rows), pl.ds(k * LANES, LANES)] = low

    def hole():
        for e in range(1, nvt):
            hole_from(e).wait_recv()
        for e in range(1, sharers):
            weights_from(e).wait_recv()
        for s in range(SUB):
            turned[...] = hole_in[pl.ds(s, rows, stride=SUB), :].T
            for j in range(GROUP):
                x = [turned[pl.ds(j * TB + n, SUB, stride=GROUP), :] for n in range(GROUP)]
                y = chunk_transpose(x, lane_chunk)
                for i in range(rows // TB):
                    flat[pl.ds((i * TB + GROUP * s + j) * SUB, SUB), :] = y[i]
        split()
        span = 2 * LANES
        for n in range(TB * TB // span):
            out = jnp.zeros((2 * rows, span), jnp.float32)
            for g in range(sharers):
                width = weights.shape[1]
                w = weights[g, :, pl.ds(n * span, span)]
                wh = w.astype(jnp.bfloat16)
                wl = (w - wh.astype(jnp.float32)).astype(jnp.bfloat16)
                b = both[:, pl.ds(g * width, width)]
                out += jnp.dot(b, wh, preferred_element_type=jnp.float32) + jnp.dot(
                    b, wl, preferred_element_type=jnp.float32
                )
            out = out[:rows] + out[rows:]
            product[pl.ds(2 * n * rows, rows), :] = out[:, :LANES]
            product[pl.ds((2 * n + 1) * rows, rows), :] = out[:, LANES:]
        for i in range(rows // TB):
            for q in range(TB // GROUP):
                x = [
                    product[pl.ds(q * rows + i * TB + n, SUB, stride=GROUP), :]
                    for n in range(GROUP)
                ]
                y = chunk_transpose(x, lane_chunk)
                for low in range(GROUP):
                    owner, r = divmod(i * TB + q * GROUP + low, local)
                    at = ((owner % members) * planes + owner // members) * local + r
                    hole_sum[pl.ds(at * SUB, SUB), :] = y[low]

    def ladder(r):
        for d in range(1, members):
            got_from(r, d).wait_recv()
        for m in range(members):
            flat[pl.ds(m * depth, depth), :] = got[r, m]
        split()
        fetch(r).wait()
        dims = (((1,), (1,)), ((), ()))
        step = 256
        for i in range(TB * TB // step):
            part = pl.ds(i * step, step)
            v = vbuf[r % 2, part, :]
            vh = v.astype(jnp.bfloat16)
            vl = (v - vh.astype(jnp.float32)).astype(jnp.bfloat16)
            b = both[...]
            total[part, :] += lax.dot_general(
                vh, b, dims, preferred_element_type=jnp.float32
            ) + lax.dot_general(vl, b, dims, preferred_element_type=jnp.float32)

        @pl.when(r + 2 < slots)
        def _():
            fetch(r + 2).start()

    def step(k, carry):
        @pl.when(k < chunks)
        def _():
            for i in range(2):
                start, count = halves[i]
                for d in range(1, planes):
                    source = (z + planes - d) % planes
                    hop1(k, i, d).wait_recv()
                    acc[
                        pl.ds(1 + k * ct + start, count),
                        pl.ds(pl.multiple_of(source * unit, unit), unit),
                        :,
                    ] = land[k, d - 1, pl.ds(start, count)]
                r = 2 * k + i

                def one(m, c):
                    stage[r, m] = acc[relay_ref[r * members + m]]
                    return c

                lax.fori_loop(0, members, one, 0)
                got[r, me] = acc[relay_ref[r * members + me]]
                for d in range(1, members):
                    hop2(r, d).start()

                @pl.when(k + 1 < chunks)
                def _():
                    for d in range(1, planes):
                        hop1(k + 1, i, d).start()

        @pl.when(k == chunks // 2)
        def _():
            hole()

        @pl.when(k > 0)
        def _():
            def one(i, c):
                ladder(2 * k - 2 + i)
                return c

            lax.fori_loop(0, 2, one, 0)

        return carry

    lax.fori_loop(0, chunks + 1, step, 0)

    for s in range(SUB):
        part = pl.ds(s * LANES, LANES)
        t = (total[part, :rows] + total[part, rows:]).T
        shares[pl.ds(s, rows, stride=SUB), :] = t + hole_sum[pl.ds(s, rows, stride=SUB), :]

    def plane_out(d):
        m = (me + d) % members
        return pltpu.make_async_remote_copy(
            src_ref=shares.at[pl.ds(pl.multiple_of(m * depth, depth), depth), :],
            dst_ref=plane_in.at[d - 1],
            send_sem=a_send.at[d - 1],
            recv_sem=a_recv.at[d - 1],
            device_id=in_plane(m),
            device_id_type=MESH,
        )

    def line_out(d):
        p = (z + d) % planes
        return pltpu.make_async_remote_copy(
            src_ref=plane_sum.at[pl.ds(pl.multiple_of(p * unit, unit), unit), :],
            dst_ref=line_in.at[d - 1],
            send_sem=b_send.at[d - 1],
            recv_sem=b_recv.at[d - 1],
            device_id=in_line(p),
            device_id_type=MESH,
        )

    for d in range(1, members):
        plane_out(d).start()
    value = shares[pl.ds(pl.multiple_of(me * depth, depth), depth), :]
    for d in range(1, members):
        plane_out(d).wait_recv()
        value += plane_in[d - 1]
    plane_sum[...] = value
    for d in range(1, planes):
        line_out(d).start()

    def drain1(k, carry):
        for i in range(2):
            for d in range(1, planes):
                hop1(k, i, d).wait_send()
        return carry

    def drain2(r, carry):
        for d in range(1, members):
            hop2(r, d).wait_send()
        return carry

    lax.fori_loop(0, chunks, drain1, 0)
    lax.fori_loop(0, slots, drain2, 0)
    for e in range(1, nvt):
        hole_out(e).wait_send()
    for e in range(1, sharers):
        weights_out(e).wait_send()
    for d in range(1, members):
        plane_out(d).wait_send()
    value = plane_sum[pl.ds(pl.multiple_of(z * unit, unit), unit), :]
    for d in range(1, planes):
        line_out(d).wait_recv()
        value += line_in[d - 1]
    final[...] = value
    for s in range(SUB):
        out_ref[:, pl.ds(s * LANES, LANES)] = final[pl.ds(s, local, stride=SUB), :]
    for d in range(1, planes):
        line_out(d).wait_send()


def exchange(
    planes, inner, ncol, chunks, ct, cap_max, tag, lists, relay, amplitudes, integrals, coupling
):
    local, wide, _ = amplitudes.shape
    slots, size, _ = integrals.shape
    members = inner * ncol
    nvt = wide // TB
    quads = wide // LANES
    unit = local * SUB
    depth = planes * unit
    rows = members * planes * local
    held_weights = coupling.shape[0]
    sharers = size // held_weights
    cfg = (planes, inner, ncol, local, slots, chunks, ct, cap_max, nvt, sharers)
    f32 = jnp.float32
    dma = pltpu.SemaphoreType.DMA
    return pl.pallas_call(
        functools.partial(exchange_kernel, cfg),
        out_shape=jax.ShapeDtypeStruct((local, size), f32),
        in_specs=[
            pl.BlockSpec(memory_space=pltpu.SMEM),
            pl.BlockSpec(memory_space=pltpu.SMEM),
            pl.BlockSpec(memory_space=pl.ANY),
            pl.BlockSpec(memory_space=pl.ANY),
            pl.BlockSpec(memory_space=pl.ANY),
        ],
        out_specs=pl.BlockSpec(memory_space=pltpu.VMEM),
        scratch_shapes=[
            pltpu.VMEM((quads * local * wide, LANES), f32),
            pltpu.VMEM((nvt * nvt, unit, LANES), f32),
            pltpu.VMEM((chunks, planes - 1, ct, unit, LANES), f32),
            pltpu.VMEM((chunks, planes - 1, ct, unit, LANES), f32),
            pltpu.VMEM((chunks * ct + 1, depth, LANES), f32),
            pltpu.VMEM((slots, members, depth, LANES), f32),
            pltpu.VMEM((slots, members, depth, LANES), f32),
            pltpu.VMEM((2, size, size), f32),
            pltpu.VMEM((rows * SUB, LANES), f32),
            pltpu.VMEM((2 * rows, size), jnp.bfloat16),
            pltpu.VMEM((size, 2 * rows), f32),
            pltpu.VMEM((rows * SUB, LANES), f32),
            pltpu.VMEM((LANES, rows), f32),
            pltpu.VMEM((sharers, held_weights, size), f32),
            pltpu.VMEM((rows * SUB, LANES), f32),
            pltpu.VMEM((rows * SUB, LANES), f32),
            pltpu.VMEM((rows * SUB, LANES), f32),
            pltpu.VMEM((members - 1, depth, LANES), f32),
            pltpu.VMEM((depth, LANES), f32),
            pltpu.VMEM((planes - 1, unit, LANES), f32),
            pltpu.VMEM((unit, LANES), f32),
            dma((quads * local,)),
            dma((chunks, 2, planes - 1)),
            dma((chunks, 2, planes - 1)),
            dma((slots, members - 1)),
            dma((slots, members - 1)),
            dma((2,)),
            dma((nvt - 1,)),
            dma((nvt - 1,)),
            dma((max(sharers - 1, 1),)),
            dma((max(sharers - 1, 1),)),
            dma(()),
            dma((members - 1,)),
            dma((members - 1,)),
            dma((planes - 1,)),
            dma((planes - 1,)),
        ],
        compiler_params=pltpu.CompilerParams(
            collective_id=tag, has_side_effects=True, vmem_limit_bytes=67043328
        ),
        name="exchange",
    )(lists, relay, amplitudes, integrals, coupling)


def tables(task_table, planes, members, z, nvt):
    slots = task_table.shape[1]
    upper, lower = task_table[:, :, 0], task_table[:, :, 1]
    ids = jnp.where(upper >= 0, upper * nvt + lower, -1).reshape(planes, members, slots)
    order = jnp.transpose(ids[:, :, ::-1], (0, 2, 1)).reshape(planes, slots * members)
    valid = (order >= 0).astype(jnp.int32)
    place = jnp.cumsum(valid, axis=1)
    fullest = jnp.max(place[:, -1])
    cap_max = slots * members
    at = jnp.arange(1, cap_max + 1, dtype=jnp.int32)
    hit = (place[:, None, :] == at[None, :, None]) & (valid[:, None, :] > 0)
    lists = jnp.sum(jnp.where(hit, order[:, None, :], 0), axis=2)
    relay = lax.dynamic_index_in_dim(place * valid, z, 0, keepdims=False)
    return lists.reshape(-1), relay, fullest


def body(amplitudes, integrals, coupling, task_table):
    nrow, ncol = lax.axis_size("row"), lax.axis_size("col")
    wide = amplitudes.shape[1]
    slots, size, _ = integrals.shape
    nvt = wide // TB
    inner = 2
    planes = nrow // inner
    members = inner * ncol
    z = lax.axis_index("row") // inner

    lists, relay, fullest = tables(task_table, planes, members, z, nvt)
    cap_max = slots * members
    mean = nvt * nvt // planes
    chunks = slots // 2
    unit = mean // chunks
    sizes = sorted({unit + -(-unit * n // 8) for n in (1, 2, 3, 4, 6, 8)})
    branches = [
        functools.partial(exchange, planes, inner, ncol, chunks, ct, cap_max, tag)
        for tag, ct in enumerate(sizes)
    ]
    limits = jnp.array([ct * chunks for ct in sizes[:-1]], jnp.int32)
    pick = jnp.sum((fullest > limits).astype(jnp.int32))
    return lax.switch(
        pick, branches, lists, relay, amplitudes, integrals, coupling.reshape(-1, size)
    )


def solution(mesh):
    in_specs = (
        P(("row", "col"), None, None),
        P(("row", "col"), None, None),
        P(("row", "col"), None, None),
        P(),
    )
    out_specs = P(("row", "col"), None)
    return jax.shard_map(body, mesh=mesh, in_specs=in_specs, out_specs=out_specs, check_vma=False)
```
